32 devices in a mesh: pool: 16 (over z, y, x), serve: 2 (over core).
Axes of the slice: x: 2, y: 2, z: 4, core: 2. Of those that a mesh axis runs over, the one named last changes fastest.
Arguments:
- queries: bfloat16 [2, 256, 73728], P('serve', None, 'pool'), may hold values from -16 to 16
- new_latent: bfloat16 [2, 147456], P('serve', 'pool'), may hold values from -8 to 8
- pool: bfloat16 [2, 192, 36864], P('serve', 'pool'), may hold values from -6 to 6
- page_owner: int32 [2, 32], P('serve'), may hold values from 0 to 15, as said below
- page_slot: int32 [2, 32], P('serve'), may hold values from 0 to 10
- new_owner: int32 [2, 4], P('serve'), may hold values from 0 to 15, as said below
- new_slot: int32 [2, 4], P('serve'), may hold values from 0 to 11
- prefix_len: int32 [2], P('serve'), may hold values from 512 to 2048, as said below
- w_uv: bfloat16 [128, 512, 128], P('pool', 'serve'), may hold values from -1 to 1
Outputs:
- attn_out: bfloat16 [2, 256, 16384], P('serve', None, 'pool')
- new_pool: bfloat16 [2, 192, 36864], P('serve', 'pool')
The draws below stay inside these ranges and needn't reach their ends.
Inputs may be any that keep to these rules, and one draw needn't show every extreme that they name: Within a request the pairs (page_owner, page_slot) differ from one another and from the pairs (new_owner, new_slot); at most 3 entries of a request's table name the same owner, and in every request some owner is named exactly 3 times. `new_owner`: the 4 new pages of a request go to different owners. `prefix_len`: some request has exactly 2048 prefix tokens.
All inputs are finite; a program needn't handle non-finite values.
Results may differ from the reference program's by a relative error of at most 0.0075.
Values may be sent and summed in bfloat16 or wider, within the bound.
A program may use at most 128 MiB of HBM per device.

```python
import jax
import jax.numpy as jnp
from jax import lax

HEADS = 128
VLAT = 512
VHEAD = 128
PAGE = 64
SUF = 256
PMAX = 2048
HOT = 3
LAT = 576
PPAGES = 32
NEWP = 4
SLOTS = 12
REQS = 2
N_POOL = 16


def drawn_pair(key):
    folded = jax.random.fold_in(key, 17)
    latent_key, query_key = jax.random.split(folded, 2)
    latent = jax.random.truncated_normal(latent_key, -6.0, 6.0, (REQS, SUF, LAT), jnp.float32)
    queries = jax.random.truncated_normal(query_key, -6.0, 6.0, (REQS, SUF, HEADS, LAT), jnp.float32)
    return (queries.reshape(REQS, SUF, HEADS * LAT), latent.reshape(REQS, SUF * LAT))


def page_tables(key):
    folded = jax.random.fold_in(key, 29)

    def per_request(request_key):
        hot_key, score_key, shuffle_key, slot_key, fresh_key = jax.random.split(request_key, 5)
        owner_key, order_key = jax.random.split(fresh_key)
        tickets = jnp.arange(N_POOL * HOT, dtype=jnp.int32)
        ticket_owner = tickets // HOT
        ticket_rank = tickets % HOT
        hottest = jax.random.randint(hot_key, (), 0, N_POOL, dtype=jnp.int32)
        ticket_score = jax.random.randint(score_key, (N_POOL * HOT,), 0, 1 << 16, dtype=jnp.int32) * (N_POOL * HOT) + tickets
        ticket_score = jnp.where(ticket_owner == hottest, tickets - N_POOL * HOT, ticket_score)
        ordering = jnp.argsort(ticket_score, stable=True)[:PPAGES].astype(jnp.int32)
        ordering = ordering[jax.random.permutation(shuffle_key, PPAGES)]
        page_owners = ticket_owner[ordering]
        page_ranks = ticket_rank[ordering]
        slot_scores = jax.random.randint(slot_key, (N_POOL, SLOTS - 1), 0, 1 << 16, dtype=jnp.int32) * SLOTS + jnp.arange(SLOTS - 1, dtype=jnp.int32)[None, :]
        small_order = jnp.argsort(slot_scores, axis=1, stable=True).astype(jnp.int32)
        last_column = jnp.full((N_POOL, 1), SLOTS - 1, jnp.int32)
        slot_order = jnp.concatenate([small_order[:, :HOT], last_column, small_order[:, HOT:]], 1).astype(jnp.int32)
        page_slots = slot_order[page_owners, page_ranks]
        others = jax.random.permutation(owner_key, N_POOL - 1)[:NEWP - 1].astype(jnp.int32)
        fresh_owners = jnp.concatenate([others, jnp.full((1,), N_POOL - 1, jnp.int32)], 0)
        fresh_owners = fresh_owners[jax.random.permutation(order_key, NEWP)].astype(jnp.int32)
        fresh_slots = slot_order[fresh_owners, HOT + jnp.arange(NEWP, dtype=jnp.int32)]
        return (page_owners, page_slots, fresh_owners, fresh_slots)
    return jax.vmap(per_request)(jax.random.split(folded, REQS))


def draw_queries(key, part):
    return drawn_pair(key)[0].astype(jnp.bfloat16)


def draw_new_latent(key, part):
    return drawn_pair(key)[1].astype(jnp.bfloat16)


def draw_page_owner(key, part):
    return page_tables(key)[0].astype(jnp.int32)


def draw_page_slot(key, part):
    return page_tables(key)[1].astype(jnp.int32)


def draw_new_owner(key, part):
    return page_tables(key)[2].astype(jnp.int32)


def draw_new_slot(key, part):
    return page_tables(key)[3].astype(jnp.int32)


def draw_prefix_len(key, part):
    length_key, top_key = jax.random.split(jax.random.fold_in(key, 41))
    lengths = jax.random.randint(length_key, (REQS,), PMAX // 4, PMAX + 1, dtype=jnp.int32)
    longest = jax.random.randint(top_key, (), 0, REQS, dtype=jnp.int32)
    return jnp.where(jnp.arange(REQS, dtype=jnp.int32) == longest, PMAX, lengths).astype(jnp.int32)


def level_of(own_key, dims, cuts, low, top_value):
    level, own = 1.0, jax.random.fold_in(own_key, 6)
    for dim, blocks in cuts:
        draws = jnp.exp(jax.random.uniform(jax.random.fold_in(own, dim), (blocks,), jnp.float32, low / len(cuts), top_value / len(cuts)))
        level = level * jnp.repeat(draws, dims[dim] // blocks).reshape([-1 if axis == dim else 1 for axis in range(len(dims))])
    return level


def bell_draw(stream_key, extent, spread, limit, pieces=(), kind=jnp.bfloat16):
    loudness = level_of(stream_key, extent, pieces, -0.22, 0.18) if pieces else 1.0
    result = jax.random.normal(stream_key, extent, jnp.float32) * spread * loudness
    return jnp.minimum(jnp.maximum(result, -limit), limit).astype(kind)


def setup_inputs(seed: int = 0) -> dict:
    seeds = jax.random.split(jax.random.key(seed), 10)
    return {
        "queries": draw_queries(jax.random.fold_in(seeds[9], 71), 0),
        "new_latent": draw_new_latent(jax.random.fold_in(seeds[9], 71), 0),
        "pool": bell_draw(seeds[2], (REQS, N_POOL * SLOTS, PAGE * LAT), 1.0, 6.0, ((0, 2), (1, 16))),
        "page_owner": draw_page_owner(jax.random.fold_in(seeds[9], 71), 0),
        "page_slot": draw_page_slot(jax.random.fold_in(seeds[9], 71), 0),
        "new_owner": draw_new_owner(jax.random.fold_in(seeds[9], 71), 0),
        "new_slot": draw_new_slot(jax.random.fold_in(seeds[9], 71), 0),
        "prefix_len": draw_prefix_len(jax.random.fold_in(seeds[9], 71), 0),
        "w_uv": bell_draw(seeds[8], (HEADS, VLAT, VHEAD), (VLAT // 16) ** -0.5, 1.0, ((0, 16), (1, 2))),
    }


softmax_scale = 192.0 ** -0.5
masked_score = -1e30


def reference(queries, new_latent, pool, page_owner, page_slot, new_owner, new_slot, prefix_len, w_uv):
    def per_request(operands):
        query_rows, latent_rows, pool_pages, owners, slot_ids, fresh_owners, fresh_slots, length = operands
        page_rows = (owners * SLOTS + slot_ids).astype(jnp.int32)
        prefix = pool_pages[page_rows].reshape(PPAGES * PAGE, LAT)
        suffix = latent_rows.reshape(SUF, LAT)
        key_rows = jnp.concatenate([prefix, suffix], 0)
        value_rows = key_rows[:, :VLAT]
        position = jnp.arange(PPAGES * PAGE, dtype=jnp.int32)
        earlier = jnp.broadcast_to(position[None, :] < length, (SUF, PPAGES * PAGE))
        query_pos = jnp.arange(SUF, dtype=jnp.int32)
        causal = query_pos[None, :] <= query_pos[:, None]
        allowed = jnp.concatenate([earlier, causal], 1)
        head_queries = query_rows.reshape(SUF, HEADS, LAT).transpose(1, 0, 2)

        def per_head(head_operands):
            one_head, head_weight = head_operands
            scores = jnp.dot(one_head, key_rows.T, preferred_element_type=jnp.float32) * softmax_scale
            scores = jnp.where(allowed, scores, masked_score)
            top_score = jnp.max(scores, axis=1, keepdims=True)
            weights = jnp.exp(scores - top_score)
            weight_sum = jnp.sum(weights, axis=1, keepdims=True)
            mixture = jnp.dot(weights.astype(jnp.bfloat16), value_rows, preferred_element_type=jnp.float32) / weight_sum
            return jnp.dot(mixture.astype(jnp.bfloat16), head_weight, preferred_element_type=jnp.float32).astype(jnp.bfloat16)

        outputs = lax.map(per_head, (head_queries, w_uv))
        attended = outputs.transpose(1, 0, 2).reshape(SUF, HEADS * VHEAD)
        targets = (fresh_owners * SLOTS + fresh_slots).astype(jnp.int32)
        updated = pool_pages.at[targets].set(latent_rows.reshape(NEWP, PAGE * LAT))
        return attended, updated

    attn_out, new_pool = lax.map(per_request, (queries, new_latent, pool, page_owner, page_slot, new_owner, new_slot, prefix_len))
    return attn_out, new_pool
```

```python
import functools

import jax
import jax.numpy as jnp
from jax import lax
from jax.experimental import pallas as pl
from jax.experimental.pallas import tpu as pltpu
from jax.sharding import PartitionSpec as P

VLAT = 512
VHEAD = 128
PAGE = 64
SUF = 256
HOT = 3
LAT = 576
PPAGES = 32
NEWP = 4
SLOTS = 12

LANES = 128
ROPE = LAT - VLAT
PAGE_ROWS = PAGE * LAT // LANES
KEYS = PPAGES * PAGE + SUF
WIDE = 640

softmax_scale = 192.0 ** (-0.5)
masked_score = -1e30
exp2_scale = softmax_scale * 1.4426950408889634

MESH = pl.DeviceIdType.MESH


def exchange_kernel(n, serve_n, block_ref, w_ref, g_ref, wg_ref,
                    z_send, z_recv, x_send, x_recv, y_send, y_recv, w_send, w_recv):
    depth = n // 4
    me = lax.axis_index("pool")
    core = lax.axis_index("serve")
    x = me % 2
    y = (me // 2) % 2
    z = me // 4
    x_peer = z * 4 + y * 2 + (1 - x)
    y_peer = z * 4 + (1 - y) * 2 + x

    barrier = pltpu.get_barrier_semaphore()
    for d in range(1, depth):
        there = ((z + d) % depth) * 4 + y * 2 + x
        pl.semaphore_signal(barrier, inc=1, device_id={"pool": there}, device_id_type=MESH)
    pl.semaphore_signal(barrier, inc=1, device_id={"pool": x_peer}, device_id_type=MESH)
    pl.semaphore_signal(barrier, inc=1, device_id={"pool": y_peer}, device_id_type=MESH)
    for d in range(1, serve_n):
        pl.semaphore_signal(
            barrier, inc=1, device_id={"serve": (core + d) % serve_n}, device_id_type=MESH
        )
    pl.semaphore_wait(barrier, depth + serve_n)

    started = []

    def send(src, dst, send_sem, recv_sem, device_id):
        copy = pltpu.make_async_remote_copy(
            src_ref=src, dst_ref=dst, send_sem=send_sem, recv_sem=recv_sem,
            device_id=device_id, device_id_type=MESH,
        )
        copy.start()
        started.append(copy)
        return copy

    order = []
    for d in range(1, depth // 2 + 1):
        order.append(d)
        if depth - d != d:
            order.append(depth - d)

    def spread(d):
        owner = ((z - d + depth) % depth) * 4 + y * 2 + x
        src = block_ref if d == 0 else g_ref.at[owner]
        x_first = send(src.at[0], g_ref.at[owner, 0], x_send.at[d, 0], x_recv.at[d, 0], {"pool": x_peer})
        y_first = send(src.at[1], g_ref.at[owner, 1], y_send.at[d, 0], y_recv.at[d, 0], {"pool": y_peer})
        x_second = send(src.at[1], g_ref.at[owner, 1], x_send.at[d, 1], x_recv.at[d, 1], {"pool": x_peer})
        y_second = send(src.at[0], g_ref.at[owner, 0], y_send.at[d, 1], y_recv.at[d, 1], {"pool": y_peer})
        return x_first, y_first, x_second, y_second

    waits = []

    def forward(d, copies):
        x_first, y_first, x_second, y_second = copies
        base = ((z - d + depth) % depth) * 4
        x_first.wait_recv()
        from_x = base + y * 2 + (1 - x)
        waits.append(send(g_ref.at[from_x, 0], g_ref.at[from_x, 0],
                          y_send.at[d, 2], y_recv.at[d, 2], {"pool": y_peer}))
        y_first.wait_recv()
        from_y = base + (1 - y) * 2 + x
        waits.append(send(g_ref.at[from_y, 1], g_ref.at[from_y, 1],
                          x_send.at[d, 2], x_recv.at[d, 2], {"pool": x_peer}))
        waits.append(x_second)
        waits.append(y_second)

    z_copies = {}
    prior = None
    first = spread(0)
    for d in order:
        there = ((z + d) % depth) * 4 + y * 2 + x
        z_copies[d] = send(block_ref, g_ref.at[me], z_send.at[d], z_recv.at[d], {"pool": there})
    for d in range(1, serve_n):
        waits.append(send(w_ref, wg_ref.at[core], w_send.at[d], w_recv.at[d],
                          {"serve": (core + d) % serve_n}))
    g_ref[pl.ds(me, 1)] = block_ref[...][None]
    wg_ref[pl.ds(core, 1)] = w_ref[...][None]
    prior = (0, first)
    for d in order:
        z_copies[d].wait_recv()
        now = spread(d)
        forward(*prior)
        prior = (d, now)
    forward(*prior)
    for copy in waits:
        copy.wait_recv()
    for copy in started:
        copy.wait_send()


def exchange(n, serve_n, block, w):
    depth = n // 4
    dma = pltpu.SemaphoreType.DMA
    vmem = pl.BlockSpec(memory_space=pltpu.VMEM)
    return pl.pallas_call(
        functools.partial(exchange_kernel, n, serve_n),
        out_shape=(
            jax.ShapeDtypeStruct((n,) + block.shape, block.dtype),
            jax.ShapeDtypeStruct((serve_n,) + w.shape, w.dtype),
        ),
        in_specs=[vmem, vmem],
        out_specs=(vmem, vmem),
        scratch_shapes=[
            dma((depth,)), dma((depth,)),
            dma((depth, 3)), dma((depth, 3)),
            dma((depth, 3)), dma((depth, 3)),
            dma((serve_n,)), dma((serve_n,)),
        ],
        compiler_params=pltpu.CompilerParams(
            collective_id=0, has_side_effects=True, vmem_limit_bytes=24 * 1024 * 1024
        ),
        name="exchange",
    )(block, w)


def attend_kernel(block_rows, owner_ref, rank_ref, length_ref, q_ref, g_ref, suffix_ref, wg_ref,
                  out_ref, keys_ref, bias_ref, causal_ref):
    @pl.when(pl.program_id(0) == 0)
    def _():
        def place(j, carry):
            base = pl.multiple_of(owner_ref[j] * block_rows + rank_ref[j] * PAGE_ROWS, 16)
            row = pl.multiple_of(j * PAGE, PAGE)
            for c in range(VLAT // LANES):
                keys_ref[pl.ds(row, PAGE), c * LANES:(c + 1) * LANES] = g_ref[pl.ds(base + c * PAGE, PAGE), :]
            rope = g_ref[pl.ds(base + PAGE * VLAT // LANES, PAGE // 2), :]
            keys_ref[pl.ds(row, PAGE // 2), VLAT:WIDE] = rope
            keys_ref[pl.ds(row + PAGE // 2, PAGE // 2), VLAT:WIDE] = jnp.concatenate(
                [rope[:, ROPE:], rope[:, :ROPE]], axis=1
            )
            return carry

        lax.fori_loop(0, PPAGES, place, 0)
        keys_ref[PPAGES * PAGE:, :] = suffix_ref[...]
        spot = lax.broadcasted_iota(jnp.int32, (8, PPAGES * PAGE), 1)
        bias_ref[...] = jnp.where(spot < length_ref[0], 0.0, masked_score)
        row = lax.broadcasted_iota(jnp.int32, (SUF, SUF), 0)
        col = lax.broadcasted_iota(jnp.int32, (SUF, SUF), 1)
        causal_ref[...] = jnp.where(col <= row, 0.0, masked_score)

    prefix = PPAGES * PAGE
    zeros = jnp.zeros((SUF, WIDE - LAT), jnp.bfloat16)
    contract_last = (((1,), (1,)), ((), ()))
    for h in range(2):
        q = jnp.concatenate([q_ref[:, h * LAT:(h + 1) * LAT], zeros], axis=1)
        s_suffix = lax.dot_general(
            q, keys_ref[prefix:, :], contract_last, preferred_element_type=jnp.float32
        ) + causal_ref[...]
        s_prefix = lax.dot_general(
            q, keys_ref[:prefix, :], contract_last, preferred_element_type=jnp.float32
        ) + bias_ref[0:1, :]
        top = jnp.maximum(
            jnp.max(s_prefix, axis=1, keepdims=True), jnp.max(s_suffix, axis=1, keepdims=True)
        )
        p_prefix = jnp.exp2((s_prefix - top) * exp2_scale)
        p_suffix = jnp.exp2((s_suffix - top) * exp2_scale)
        total = jnp.sum(p_prefix, axis=1, keepdims=True) + jnp.sum(p_suffix, axis=1, keepdims=True)
        mixed = jnp.dot(
            p_prefix.astype(jnp.bfloat16), keys_ref[:prefix, :VLAT], preferred_element_type=jnp.float32
        ) + jnp.dot(
            p_suffix.astype(jnp.bfloat16), keys_ref[prefix:, :VLAT], preferred_element_type=jnp.float32
        )
        mixed = (mixed / total).astype(jnp.bfloat16)
        w = wg_ref[:, h].reshape(VLAT, VHEAD)
        out_ref[:, h * VHEAD:(h + 1) * VHEAD] = jnp.dot(
            mixed, w, preferred_element_type=jnp.float32
        ).astype(jnp.bfloat16)


def attend(block_rows, owners, ranks, length, queries, gathered, suffix, w_all):
    heads = queries.shape[1] // LAT
    serve_n, w_rows = w_all.shape[0], w_all.shape[2]
    whole = lambda shape: pl.BlockSpec(shape, lambda i, *_: (0,) * len(shape))
    return pl.pallas_call(
        functools.partial(attend_kernel, block_rows),
        out_shape=jax.ShapeDtypeStruct((SUF, heads * VHEAD), jnp.bfloat16),
        grid_spec=pltpu.PrefetchScalarGridSpec(
            num_scalar_prefetch=3,
            grid=(heads // 2,),
            in_specs=[
                pl.BlockSpec((SUF, 2 * LAT), lambda i, *_: (0, i)),
                whole(gathered.shape),
                whole(suffix.shape),
                pl.BlockSpec((serve_n, 2, w_rows, VHEAD), lambda i, *_: (0, i, 0, 0)),
            ],
            out_specs=pl.BlockSpec((SUF, 2 * VHEAD), lambda i, *_: (0, i)),
            scratch_shapes=[
                pltpu.VMEM((KEYS, WIDE), jnp.bfloat16),
                pltpu.VMEM((8, PPAGES * PAGE), jnp.float32),
                pltpu.VMEM((SUF, SUF), jnp.float32),
            ],
        ),
        compiler_params=pltpu.CompilerParams(vmem_limit_bytes=48 * 1024 * 1024),
        name="attend",
    )(owners, ranks, length, queries, gathered, suffix, w_all)


def local(n, serve_n, queries, new_latent, pool, page_owner, page_slot, new_owner, new_slot,
          prefix_len, w_uv):
    holder = lax.axis_index("pool")
    owners = page_owner[0]
    slot_ids = page_slot[0]
    local_pages = pool[0]
    page_index = jnp.arange(PPAGES, dtype=jnp.int32)
    earlier = (page_index[None, :] < page_index[:, None]) & (owners[None, :] == owners[:, None])
    ranks = jnp.sum(earlier.astype(jnp.int32), axis=1)
    my_ranks = jnp.arange(HOT, dtype=jnp.int32)
    my_rows = (owners[None, :] == holder) & (ranks[None, :] == my_ranks[:, None])
    slot_rows = jnp.sum(jnp.where(my_rows, slot_ids[None, :], 0), axis=1)

    pages = local_pages[slot_rows].reshape(HOT, PAGE, LAT)
    latent = pages[:, :, :VLAT].reshape(HOT, PAGE, VLAT // LANES, LANES).transpose(0, 2, 1, 3)
    latent = latent.reshape(HOT, PAGE * VLAT // LANES, LANES)
    rope = pages[:, :, VLAT:].reshape(HOT, 2, PAGE // 2, ROPE).transpose(0, 2, 1, 3)
    rope = rope.reshape(HOT, PAGE // 2, LANES)
    packed = jnp.concatenate([latent, rope], axis=1).reshape(HOT * PAGE_ROWS, LANES)
    fresh = new_latent.reshape(-1, LANES)
    used = HOT * PAGE_ROWS + fresh.shape[0]
    block_rows = -(-used // 32) * 32
    filler = jnp.zeros((block_rows - used, LANES), jnp.bfloat16)
    block = jnp.concatenate([packed, fresh, filler], axis=0).reshape(2, block_rows // 2, LANES)

    gathered, w_all = exchange(n, serve_n, block, w_uv)
    by_owner = gathered.reshape(n, block_rows, LANES)
    suffix_flat = by_owner[:, HOT * PAGE_ROWS:used]
    suffix = jnp.pad(suffix_flat.reshape(SUF, LAT), ((0, 0), (0, WIDE - LAT)))
    attended = attend(
        block_rows, owners, ranks, prefix_len, queries[0],
        gathered.reshape(n * block_rows, LANES), suffix, w_all,
    )

    fresh_pages = suffix_flat.reshape(NEWP, PAGE * LAT)
    placing = (jnp.arange(SLOTS, dtype=jnp.int32)[:, None] == new_slot[0][None, :]) & (
        new_owner[0][None, :] == holder
    )
    written = jnp.dot(
        placing.astype(jnp.bfloat16), fresh_pages, preferred_element_type=jnp.float32
    ).astype(jnp.bfloat16)
    updated = jnp.where(jnp.any(placing, axis=1)[:, None], written, local_pages)
    return (attended[None], updated[None])


def solution(mesh):
    in_specs = (
        P("serve", None, "pool"),
        P("serve", "pool"),
        P("serve", "pool", None),
        P("serve", None),
        P("serve", None),
        P("serve", None),
        P("serve", None),
        P("serve"),
        P("pool", "serve", None),
    )
    out_specs = (P("serve", None, "pool"), P("serve", "pool", None))
    body = functools.partial(local, mesh.shape["pool"], mesh.shape["serve"])
    return jax.shard_map(body, mesh=mesh, in_specs=in_specs, out_specs=out_specs, check_vma=False)
```

```python
import functools

import jax
import jax.numpy as jnp
from jax import lax
from jax.experimental import pallas as pl
from jax.experimental.pallas import tpu as pltpu
from jax.sharding import PartitionSpec as P

VLAT = 512
VHEAD = 128
PAGE = 64
SUF = 256
HOT = 3
LAT = 576
PPAGES = 32
NEWP = 4
SLOTS = 12

LANES = 128
ROPE = LAT - VLAT
PAGE_ROWS = PAGE * LAT // LANES
KEYS = PPAGES * PAGE + SUF
WIDE = 640

softmax_scale = 192.0 ** (-0.5)
masked_score = -1e30
exp2_scale = softmax_scale * 1.4426950408889634

MESH = pl.DeviceIdType.MESH


def fused_kernel(n, serve_n, tokens, block_ref, w_ref, q_ref, count_ref, out_ref, suffix_ref,
                 g_ref, wg_ref, qs_ref, k_ref, stage_ref, acc_ref, top_ref, sum_ref,
                 z_send, z_recv, x_send, x_recv, y_send, y_recv, w_send, w_recv):
    depth = n // 4
    heads = q_ref.shape[1] // LAT
    half = block_ref.shape[0] // 2
    me = lax.axis_index("pool")
    core = lax.axis_index("serve")
    x = me % 2
    y = (me // 2) % 2
    z = me // 4
    x_peer = z * 4 + y * 2 + (1 - x)
    y_peer = z * 4 + (1 - y) * 2 + x

    barrier = pltpu.get_barrier_semaphore()
    for d in range(1, depth):
        there = ((z + d) % depth) * 4 + y * 2 + x
        pl.semaphore_signal(barrier, inc=1, device_id={"pool": there}, device_id_type=MESH)
    pl.semaphore_signal(barrier, inc=1, device_id={"pool": x_peer}, device_id_type=MESH)
    pl.semaphore_signal(barrier, inc=1, device_id={"pool": y_peer}, device_id_type=MESH)
    for d in range(1, serve_n):
        pl.semaphore_signal(
            barrier, inc=1, device_id={"serve": (core + d) % serve_n}, device_id_type=MESH
        )
    pl.semaphore_wait(barrier, depth + serve_n)

    started = []

    def send(src, dst, send_sem, recv_sem, device_id):
        copy = pltpu.make_async_remote_copy(
            src_ref=src, dst_ref=dst, send_sem=send_sem, recv_sem=recv_sem,
            device_id=device_id, device_id_type=MESH,
        )
        copy.start()
        started.append(copy)
        return copy

    order = []
    for d in range(1, depth // 2 + 1):
        order.append(d)
        if depth - d != d:
            order.append(depth - d)

    def base_of(d):
        return ((z - d + depth) % depth) * 4

    def part(ref, i):
        return ref.at[pl.ds(i * half, half)]

    arrivals = {}

    def spread(d):
        owner = base_of(d) + y * 2 + x
        src = block_ref if d == 0 else g_ref.at[owner]
        dst = g_ref.at[owner]
        arrivals[d] = [
            send(part(src, 0), part(dst, 0), x_send.at[d, 0], x_recv.at[d, 0], {"pool": x_peer}),
            send(part(src, 1), part(dst, 1), y_send.at[d, 0], y_recv.at[d, 0], {"pool": y_peer}),
            send(part(src, 1), part(dst, 1), x_send.at[d, 1], x_recv.at[d, 1], {"pool": x_peer}),
            send(part(src, 0), part(dst, 0), y_send.at[d, 1], y_recv.at[d, 1], {"pool": y_peer}),
        ]

    def forward(d):
        x_first, y_first, x_second, y_second = arrivals[d]
        x_first.wait_recv()
        over = part(g_ref.at[base_of(d) + y * 2 + (1 - x)], 0)
        to_y = send(over, over, y_send.at[d, 2], y_recv.at[d, 2], {"pool": y_peer})
        y_first.wait_recv()
        over = part(g_ref.at[base_of(d) + (1 - y) * 2 + x], 1)
        to_x = send(over, over, x_send.at[d, 2], x_recv.at[d, 2], {"pool": x_peer})
        arrivals[d] = [x_second, y_second, to_y, to_x]

    spread(0)
    z_copies = {}
    for d in order:
        there = ((z + d) % depth) * 4 + y * 2 + x
        z_copies[d] = send(block_ref, g_ref.at[me], z_send.at[d], z_recv.at[d], {"pool": there})
    w_copies = [
        send(w_ref, wg_ref.at[core], w_send.at[d], w_recv.at[d], {"serve": (core + d) % serve_n})
        for d in range(1, serve_n)
    ]

    pending = []

    def advance(d):
        def step():
            z_copies[d].wait_recv()
            spread(d)
        return step

    pending.append(lambda: forward(0))
    for d in order:
        pending.append(advance(d))
        pending.append(functools.partial(forward, d))

    def communicate(steps):
        for _ in range(min(steps, len(pending))):
            pending.pop(0)()

    g_ref[pl.ds(me, 1)] = block_ref[...][None]
    wg_ref[pl.ds(core, 1)] = w_ref[...][None]
    unit = jnp.where(
        lax.broadcasted_iota(jnp.int32, (SUF, WIDE - LAT), 1) == 0, 1.0, 0.0
    ).astype(jnp.bfloat16)
    for h in range(heads):
        qs_ref[h * SUF:(h + 1) * SUF, :] = jnp.concatenate(
            [q_ref[:, h * LAT:(h + 1) * LAT], unit], axis=1
        )

    lane = lax.broadcasted_iota(jnp.int32, (PAGE // 2, LANES), 1)
    line = lax.broadcasted_iota(jnp.int32, (PAGE // 2, LANES), 0)

    def unpack(d):
        def place(i, carry):
            owner = base_of(d) + i // HOT
            rank = i % HOT
            base = pl.multiple_of(rank * PAGE_ROWS, 16)
            row = pl.multiple_of(i * PAGE, PAGE)
            for c in range(VLAT // LANES):
                k_ref[pl.ds(row, PAGE), c * LANES:(c + 1) * LANES] = g_ref[
                    owner, pl.ds(base + c * PAGE, PAGE), :]
            rope = g_ref[owner, pl.ds(base + PAGE * VLAT // LANES, PAGE // 2), :].astype(jnp.float32)
            count = count_ref[owner * HOT + rank]
            swapped = jnp.concatenate([rope[:, ROPE:], rope[:, :ROPE]], axis=1)
            for k, values in enumerate((rope, swapped)):
                absent = (lane == ROPE) & (line + k * (PAGE // 2) >= count)
                tile = jnp.where(lane < ROPE, values, jnp.where(absent, masked_score, 0.0))
                k_ref[pl.ds(row + k * (PAGE // 2), PAGE // 2), VLAT:WIDE] = tile.astype(jnp.bfloat16)
            return carry

        lax.fori_loop(0, 4 * HOT, place, 0)

    tile_rows = 2 * SUF
    tiles = heads // 2
    contract_last = (((1,), (1,)), ((), ()))

    def absorb(keys_ref, low, high, first, causal):
        def tile(t, carry):
            rows = pl.ds(pl.multiple_of(t * tile_rows, tile_rows), tile_rows)
            keys = keys_ref[...]
            scores = lax.dot_general(
                qs_ref[rows, :], keys, contract_last, preferred_element_type=jnp.float32
            )
            if causal:
                row = lax.broadcasted_iota(jnp.int32, scores.shape, 0) % SUF
                col = lax.broadcasted_iota(jnp.int32, scores.shape, 1)
                scores = jnp.where(col <= row, scores, masked_score)
            top = jnp.max(scores, axis=1, keepdims=True)
            if not first:
                before = top_ref[rows, :1]
                top = jnp.maximum(top, before)
            shift = top * exp2_scale
            weights = jnp.exp2(scores * exp2_scale - shift)
            total = jnp.sum(weights, axis=1, keepdims=True)
            mixed = jnp.dot(
                weights.astype(jnp.bfloat16), keys[:, :VLAT], preferred_element_type=jnp.float32
            )
            if not first:
                rescale = jnp.exp2((before - top) * exp2_scale)
                total = total + sum_ref[rows, :1] * rescale
                mixed = mixed + acc_ref[rows, :] * rescale
            top_ref[rows, :] = jnp.broadcast_to(top, (tile_rows, LANES))
            sum_ref[rows, :] = jnp.broadcast_to(total, (tile_rows, LANES))
            acc_ref[rows, :] = mixed
            return carry

        lax.fori_loop(low, high, tile, 0)

    communicate(2)
    for k, d in enumerate([0] + order):
        while len(arrivals[d]) != 4 or (len(pending) > 2 * (len(order) - k) and pending):
            communicate(1)
        for copy in arrivals[d]:
            copy.wait_recv()
        unpack(d)
        absorb(k_ref, 0, tiles // 2, k == 0, False)
        communicate(2)
        absorb(k_ref, tiles // 2, tiles, k == 0, False)
        communicate(2)

    base = HOT * PAGE_ROWS

    def place_suffix(o, carry):
        rows = pl.ds(pl.multiple_of(o * tokens, 8), tokens)
        for c in range(VLAT // LANES):
            stage_ref[rows, c * LANES:(c + 1) * LANES] = g_ref[
                o, base + c * tokens:base + (c + 1) * tokens, :].astype(jnp.float32)
        at = base + tokens * VLAT // LANES
        rope = g_ref[o, at:at + tokens // 2, :].astype(jnp.float32)
        swapped = jnp.concatenate([rope[:, ROPE:], rope[:, :ROPE]], axis=1)
        both = jnp.concatenate([rope, swapped], axis=0)
        keep = lax.broadcasted_iota(jnp.int32, (tokens, LANES), 1) < ROPE
        stage_ref[rows, VLAT:WIDE] = jnp.where(keep, both, 0.0)
        return carry

    lax.fori_loop(0, n, place_suffix, 0)
    suffix_ref[...] = stage_ref[...].astype(jnp.bfloat16)
    absorb(suffix_ref, 0, tiles, False, True)
    for copy in w_copies:
        copy.wait_recv()
    for h in range(heads):
        rows = slice(h * SUF, (h + 1) * SUF)
        mixed = (acc_ref[rows, :] / sum_ref[rows, :1]).astype(jnp.bfloat16)
        out_ref[:, h * VHEAD:(h + 1) * VHEAD] = jnp.dot(
            mixed, wg_ref[:, h].reshape(VLAT, VHEAD), preferred_element_type=jnp.float32
        ).astype(jnp.bfloat16)
    for copy in started:
        copy.wait_send()


def fused(n, serve_n, tokens, block, w, queries, counts):
    depth = n // 4
    heads = queries.shape[1] // LAT
    dma = pltpu.SemaphoreType.DMA
    vmem = pl.BlockSpec(memory_space=pltpu.VMEM)
    return pl.pallas_call(
        functools.partial(fused_kernel, n, serve_n, tokens),
        out_shape=(
            jax.ShapeDtypeStruct((SUF, heads * VHEAD), jnp.bfloat16),
            jax.ShapeDtypeStruct((SUF, WIDE), jnp.bfloat16),
        ),
        in_specs=[vmem, vmem, vmem, pl.BlockSpec(memory_space=pltpu.SMEM)],
        out_specs=(vmem, vmem),
        scratch_shapes=[
            pltpu.VMEM((n,) + block.shape, jnp.bfloat16),
            pltpu.VMEM((serve_n,) + w.shape, jnp.bfloat16),
            pltpu.VMEM((heads * SUF, WIDE), jnp.bfloat16),
            pltpu.VMEM((4 * HOT * PAGE, WIDE), jnp.bfloat16),
            pltpu.VMEM((SUF, WIDE), jnp.float32),
            pltpu.VMEM((heads * SUF, VLAT), jnp.float32),
            pltpu.VMEM((heads * SUF, LANES), jnp.float32),
            pltpu.VMEM((heads * SUF, LANES), jnp.float32),
            dma((depth,)), dma((depth,)),
            dma((depth, 3)), dma((depth, 3)),
            dma((depth, 3)), dma((depth, 3)),
            dma((serve_n,)), dma((serve_n,)),
        ],
        compiler_params=pltpu.CompilerParams(
            collective_id=0, has_side_effects=True, vmem_limit_bytes=48 * 1024 * 1024
        ),
        name="fused",
    )(block, w, queries, counts)


def local(n, serve_n, queries, new_latent, pool, page_owner, page_slot, new_owner, new_slot,
          prefix_len, w_uv):
    holder = lax.axis_index("pool")
    owners = page_owner[0]
    slot_ids = page_slot[0]
    local_pages = pool[0]
    page_index = jnp.arange(PPAGES, dtype=jnp.int32)
    earlier = (page_index[None, :] < page_index[:, None]) & (owners[None, :] == owners[:, None])
    ranks = jnp.sum(earlier.astype(jnp.int32), axis=1)
    my_ranks = jnp.arange(HOT, dtype=jnp.int32)
    my_rows = (owners[None, :] == holder) & (ranks[None, :] == my_ranks[:, None])
    slot_rows = jnp.sum(jnp.where(my_rows, slot_ids[None, :], 0), axis=1)

    pages = local_pages[slot_rows].reshape(HOT, PAGE, LAT)
    latent = pages[:, :, :VLAT].reshape(HOT, PAGE, VLAT // LANES, LANES).transpose(0, 2, 1, 3)
    latent = latent.reshape(HOT, PAGE * VLAT // LANES, LANES)
    rope = pages[:, :, VLAT:].reshape(HOT, 2, PAGE // 2, ROPE).transpose(0, 2, 1, 3)
    rope = rope.reshape(HOT, PAGE // 2, LANES)
    packed = jnp.concatenate([latent, rope], axis=1).reshape(HOT * PAGE_ROWS, LANES)
    fresh = new_latent.reshape(-1, LAT)
    tokens = fresh.shape[0]
    fresh_latent = fresh[:, :VLAT].reshape(tokens, VLAT // LANES, LANES).transpose(1, 0, 2)
    fresh_rope = fresh[:, VLAT:].reshape(2, tokens // 2, ROPE).transpose(1, 0, 2)
    used = HOT * PAGE_ROWS + tokens * LAT // LANES
    block_rows = -(-used // 32) * 32
    filler = jnp.zeros((block_rows - used, LANES), jnp.bfloat16)
    block = jnp.concatenate(
        [packed, fresh_latent.reshape(-1, LANES), fresh_rope.reshape(-1, LANES), filler], axis=0
    )
    spots = jnp.arange(n * HOT, dtype=jnp.int32)
    held = jnp.clip(prefix_len[0] - PAGE * page_index, 0, PAGE)
    counts = jnp.sum(
        jnp.where(spots[:, None] == (owners * HOT + ranks)[None, :], held[None, :], 0), axis=1
    )
    attended, suffix = fused(n, serve_n, tokens, block, w_uv, queries[0], counts)
    fresh_pages = suffix[:, :LAT].reshape(NEWP, PAGE * LAT)
    placing = (jnp.arange(SLOTS, dtype=jnp.int32)[:, None] == new_slot[0][None, :]) & (
        new_owner[0][None, :] == holder
    )
    written = jnp.dot(
        placing.astype(jnp.bfloat16), fresh_pages, preferred_element_type=jnp.float32
    ).astype(jnp.bfloat16)
    updated = jnp.where(jnp.any(placing, axis=1)[:, None], written, local_pages)
    return (attended[None], updated[None])


def solution(mesh):
    in_specs = (
        P("serve", None, "pool"),
        P("serve", "pool"),
        P("serve", "pool", None),
        P("serve", None),
        P("serve", None),
        P("serve", None),
        P("serve", None),
        P("serve"),
        P("pool", "serve", None),
    )
    out_specs = (P("serve", None, "pool"), P("serve", "pool", None))
    body = functools.partial(local, mesh.shape["pool"], mesh.shape["serve"])
    return jax.shard_map(body, mesh=mesh, in_specs=in_specs, out_specs=out_specs, check_vma=False)
```
